128 devices in a mesh: data: 1, pp: 2 (over core), ep: 64 (over z, y, x).
Axes of the slice: x: 4, y: 4, z: 4, core: 2. Of those that a mesh axis runs over, the one named last changes fastest.
Arguments:
- expert_out: bfloat16 [2, 64, 1536, 2048], P(('data', 'pp'), 'ep')
- expert_ids: int32 [2, 192, 48, 6], P(('data', 'pp'), 'ep')
- slot_ids: int32 [2, 192, 48, 6], P(('data', 'pp'), 'ep')
- gate_vals: float32 [2, 192, 48, 6], P(('data', 'pp'), 'ep')
- residual: bfloat16 [2, 192, 48, 2048], P(('data', 'pp'), 'ep')
- norm_scale: float32 [2, 2048], P('pp')
- w_query: bfloat16 [2, 2048, 16, 128], P('pp')
- w_key: bfloat16 [2, 2048, 16, 128], P('pp')
- w_value: bfloat16 [2, 2048, 16, 128], P('pp')
- w_out: bfloat16 [2, 16, 128, 2048], P('pp')
Outputs:
- output: bfloat16 [2, 192, 48, 2048], P(('data', 'pp'), 'ep')
All inputs are finite; a program needn't handle non-finite values.
Results may differ from the reference program's by a relative error of at most 0.02.
Values are sent between devices in bfloat16 or wider.
A program may use at most 1 GiB of HBM per device.

```python
import jax
import jax.numpy as jnp
from jax import lax

STAGES = 2
EP_DEVS = 64
SEQS_DEV = 3
SEQ_LEN = 48
D = 2048
HEADS = 16
HEAD = 128
EXPERTS = 64
TOP = 6
CAP_DEV = 24

NUM_SEQ = EP_DEVS * SEQS_DEV
TOKENS = NUM_SEQ * SEQ_LEN
TOK_DEV = SEQS_DEV * SEQ_LEN
CAPACITY = EP_DEVS * CAP_DEV
HIDDEN = HEADS * HEAD
NORM_EPS = 1e-6


def queue_pos(flat_ids):
    sort_order = jnp.argsort(flat_ids, stable=True)
    ordered = flat_ids[sort_order]
    first_pos = jnp.searchsorted(ordered, ordered, side='left')
    rank_sorted = jnp.arange(flat_ids.shape[0]) - first_pos
    return rank_sorted[jnp.argsort(sort_order, stable=True)]


def draw_routing(route_key):
    rank_key, noise_key = jax.random.split(route_key)
    rank_draw = jax.random.randint(rank_key, (STAGES, EXPERTS), 0, 1 << 20) * EXPERTS + jnp.arange(EXPERTS)
    expert_rank = jnp.argsort(rank_draw, axis=-1)
    hot_bias = jnp.where(expert_rank == 0, 4000, jnp.where(expert_rank < 3, 200, 0))
    stage_keys = jax.random.split(noise_key, STAGES)

    def pick_stage(stage_args):
        stage_key, stage_bias = stage_args
        score_noise = jax.random.randint(stage_key, (TOKENS, EXPERTS), 0, 1000)
        score_total = (score_noise + stage_bias) * EXPERTS + jnp.arange(EXPERTS)
        return lax.top_k(score_total, TOP)[1]

    expert_ids = lax.map(pick_stage, (stage_keys, hot_bias)).astype(jnp.int32)
    positions = jax.vmap(queue_pos)(expert_ids.reshape(STAGES * EP_DEVS, TOK_DEV * TOP))
    positions = positions.reshape(STAGES, NUM_SEQ, SEQ_LEN, TOP)
    owner_dev = (jnp.arange(NUM_SEQ) // SEQS_DEV)[None, :, None, None]
    slot_ids = jnp.where(positions < CAP_DEV, owner_dev * CAP_DEV + positions, -1).astype(jnp.int32)
    return expert_ids.reshape(STAGES, NUM_SEQ, SEQ_LEN, TOP), slot_ids


def setup_inputs(seed: int = 0, part: int = 0) -> dict:
    base_key = jax.random.key(seed)
    part_key = jax.random.fold_in(base_key, part)
    route_key, out_key, gain_key, mean_key, gate_key, resid_key = jax.random.split(part_key, 6)
    norm_key, q_key, k_key, v_key, o_key = jax.random.split(base_key, 5)
    expert_ids, slot_ids = draw_routing(route_key)
    expert_gain = jnp.exp(0.6 * jax.random.normal(gain_key, (STAGES, EXPERTS, 1, 1), jnp.float32))
    expert_mean = 0.7 * jax.random.normal(mean_key, (STAGES, EXPERTS, 1, D), jnp.float32)
    expert_out = (expert_mean + expert_gain * jax.random.normal(out_key, (STAGES, EXPERTS, CAPACITY, D), jnp.float32)).astype(jnp.bfloat16)
    gate_vals = jax.nn.softmax(2.0 * jax.random.normal(gate_key, (STAGES, NUM_SEQ, SEQ_LEN, TOP), jnp.float32), axis=-1).astype(jnp.float32)
    residual = jax.random.normal(resid_key, (STAGES, NUM_SEQ, SEQ_LEN, D), jnp.float32).astype(jnp.bfloat16)
    norm_scale = jnp.exp(0.5 * jax.random.normal(norm_key, (STAGES, D), jnp.float32)).astype(jnp.float32)
    w_query = (1.3 * D ** -0.5 * jax.random.normal(q_key, (STAGES, D, HEADS, HEAD), jnp.float32)).astype(jnp.bfloat16)
    w_key = (1.3 * D ** -0.5 * jax.random.normal(k_key, (STAGES, D, HEADS, HEAD), jnp.float32)).astype(jnp.bfloat16)
    w_value = (D ** -0.5 * jax.random.normal(v_key, (STAGES, D, HEADS, HEAD), jnp.float32)).astype(jnp.bfloat16)
    w_out = (3.0 * HIDDEN ** -0.5 * jax.random.normal(o_key, (STAGES, HEADS, HEAD, D), jnp.float32)).astype(jnp.bfloat16)
    return {'expert_out': expert_out, 'expert_ids': expert_ids, 'slot_ids': slot_ids, 'gate_vals': gate_vals, 'residual': residual, 'norm_scale': norm_scale, 'w_query': w_query, 'w_key': w_key, 'w_value': w_value, 'w_out': w_out}


def combine_rows(expert_table, ids_seq, slots_seq, gates_seq, resid_seq):
    kept_mask = slots_seq >= 0
    picked_rows = expert_table[ids_seq, jnp.where(kept_mask, slots_seq, 0)].astype(jnp.float32)
    gate_used = jnp.where(kept_mask, gates_seq, 0.0)
    merged = resid_seq.astype(jnp.float32) + jnp.sum(gate_used[..., None] * picked_rows, axis=1)
    return merged.astype(jnp.bfloat16)


def attn_block(merged, scale_vec, q_mat, k_mat, v_mat, o_mat):
    resid_f32 = merged.astype(jnp.float32)
    inv_rms = lax.rsqrt(jnp.mean(resid_f32 * resid_f32, axis=-1, keepdims=True) + NORM_EPS)
    normed_in = (resid_f32 * inv_rms * scale_vec).astype(jnp.bfloat16)

    def project(w_mat):
        product = jnp.dot(normed_in, w_mat, preferred_element_type=jnp.float32).astype(jnp.bfloat16)
        return product.reshape(SEQ_LEN, HEADS, HEAD).astype(jnp.float32)

    q_heads = project(q_mat)
    k_heads = project(k_mat)
    v_heads = project(v_mat)
    scores = jnp.einsum('qhe,khe->hqk', q_heads, k_heads) * HEAD ** -0.5
    causal = jnp.arange(SEQ_LEN)[:, None] >= jnp.arange(SEQ_LEN)[None, :]
    scores = jnp.where(causal, scores, -1e30)
    exp_scores = jnp.exp(scores - jnp.max(scores, axis=-1, keepdims=True))
    row_sums = jnp.sum(exp_scores, axis=-1)
    mixed_vals = jnp.einsum('hqk,khe->qhe', exp_scores.astype(jnp.bfloat16).astype(jnp.float32), v_heads)
    attn_out = (mixed_vals / row_sums.T[:, :, None]).astype(jnp.bfloat16).reshape(SEQ_LEN, HIDDEN)
    proj_out = jnp.dot(attn_out, o_mat, preferred_element_type=jnp.float32).astype(jnp.bfloat16)
    return (resid_f32 + proj_out.astype(jnp.float32)).astype(jnp.bfloat16)


def reference(expert_out, expert_ids, slot_ids, gate_vals, residual, norm_scale, w_query, w_key, w_value, w_out):
    def one_stage(stage_idx):
        prev_stage = (stage_idx + STAGES - 1) % STAGES
        expert_table = expert_out[prev_stage]
        scale_vec = norm_scale[stage_idx]
        q_mat = w_query[stage_idx].reshape(D, HIDDEN)
        k_mat = w_key[stage_idx].reshape(D, HIDDEN)
        v_mat = w_value[stage_idx].reshape(D, HIDDEN)
        o_mat = w_out[stage_idx].reshape(HIDDEN, D)

        def one_seq(seq_idx):
            merged = combine_rows(expert_table, expert_ids[prev_stage, seq_idx], slot_ids[prev_stage, seq_idx], gate_vals[prev_stage, seq_idx], residual[prev_stage, seq_idx])
            return attn_block(merged, scale_vec, q_mat, k_mat, v_mat, o_mat)

        return lax.map(one_seq, jnp.arange(NUM_SEQ))

    return lax.map(one_stage, jnp.arange(STAGES))
```

```python
import jax
import jax.numpy as jnp
from jax import lax
from jax.experimental import pallas as pl
from jax.experimental.pallas import tpu as pltpu
from jax.sharding import PartitionSpec as P

NORM_EPS = 1e-6
MESH = pl.DeviceIdType.MESH
ORDERS = ((2, 1, 0), (1, 0, 2), (0, 2, 1))
UNITS = ((0, 0, 512), (1, 768, 384), (2, 1408, 384), (0, 512, 256), (1, 1152, 256), (2, 1792, 256))
LENGTH = 48


def stage_kernel(o_ref, ids_ref, slots_ref, gates_ref, resid_ref, scale_ref, wq_ref, wk_ref, wv_ref, wo_ref, z_ref,
                 tq_ref, tk_ref, tv_ref, to_ref, ids, slots, gates, resid, g_buf, y_buf, x_buf, a_buf, turn,
                 ra, rc, s1, s2, s3, in1, in2, in3, sems):
    f32, bf = jnp.float32, jnp.bfloat16
    me = lax.axis_index('ep')
    core = lax.axis_index('pp')
    other = 1 - core
    m = (me // 16, (me // 4) % 4, me % 4)
    tokens, width = resid_ref.shape
    cap = o_ref.shape[3]
    n_seq, top_k = ids_ref.shape[:2]
    half = tokens // 2
    sa, xa, so, xo, sb, xb, s_two, x_two, s_one, x_one, sm, xm, sr, xr, sw = sems

    def shift(order, deltas):
        c = list(m)
        for ax, d in zip(order, deltas):
            c[ax] = (c[ax] + d) % 4
        return c

    def flat(c):
        return c[0] * 16 + c[1] * 4 + c[2]

    def dev(c, core_id):
        return {'pp': core_id, 'ep': flat(c)}

    def far(i):
        return 1 + (2 * i) % 3

    def loop(n, step):
        lax.fori_loop(0, n, lambda i, _: (step(i), 0)[1], 0)

    fetches = [pltpu.make_async_copy(w, t, sw.at[i]) for i, (w, t) in enumerate(((wq_ref, tq_ref), (wk_ref, tk_ref), (wv_ref, tv_ref), (wo_ref, to_ref)))]
    for fetch in fetches:
        fetch.start()

    barrier = pltpu.get_barrier_semaphore()

    def greet(i):
        for ax in range(3):
            for cid in (core, other):
                pl.semaphore_signal(barrier, inc=1, device_id=dev(shift((ax,), (i + 1,)), cid), device_id_type=MESH)

    loop(3, greet)
    pl.semaphore_signal(barrier, inc=1, device_id=dev(m, other), device_id_type=MESH)
    pl.semaphore_wait(barrier, 19)

    def osrc(u, a, b):
        col, first, wide = UNITS[u]
        order = ORDERS[col]
        idx = [slice(None)] * 3
        idx[order[0]] = a
        idx[order[1]] = b
        return o_ref.at[idx[0], idx[1], idx[2], :, pl.ds(first, wide)]

    def remote(src, dst, send, recv, c, core_id):
        return pltpu.make_async_remote_copy(src_ref=src, dst_ref=dst, send_sem=send, recv_sem=recv, device_id=dev(c, core_id), device_id_type=MESH)

    def cp_a(u, da, db):
        order = ORDERS[UNITS[u][0]]
        c = shift(order, (da, db, 0))
        return remote(osrc(u, c[order[0]], c[order[1]]), ra[u].at[da - 1, db - 1], sa.at[u, da - 1, db], xa.at[u, da - 1, db],
                      shift(order, (da, 0, 0)), other)

    def cp_a0(u, da):
        order = ORDERS[UNITS[u][0]]
        c = shift(order, (da, 0, 0))
        return remote(osrc(u, c[order[0]], c[order[1]]), rc[u].at[:, da * 4], sa.at[u, da - 1, 0], xa.at[u, da - 1, 0], c, other)

    def cp_own(u):
        order = ORDERS[UNITS[u][0]]
        return remote(osrc(u, m[order[0]], m[order[1]]), rc[u].at[:, 0], so.at[u], xo.at[u], m, other)

    def cp_b(u, da, db):
        return remote(ra[u].at[da - 1, db - 1], rc[u].at[:, da * 4 + db], sb.at[u, da, db - 1], xb.at[u, da, db - 1],
                      shift(ORDERS[UNITS[u][0]], (0, db, 0)), core)

    def cp_b0(u, db):
        order = ORDERS[UNITS[u][0]]
        c = shift(order, (0, db, 0))
        return remote(osrc(u, c[order[0]], c[order[1]]), rc[u].at[:, db], sb.at[u, 0, db - 1], xb.at[u, 0, db - 1], c, other)

    def line(u, d):
        return shift(ORDERS[UNITS[u][0]], (0, 0, d))

    def cp_two(u, way):
        return remote(s2[u].at[pl.ds(way * half, half)], in2[u].at[way], s_two.at[u, way], x_two.at[u, way], line(u, (1, 3)[way]), core)

    def cp_one(u, way):
        return remote((s1, s3)[way][u], (in1, in3)[way][u], s_one.at[u, way], x_one.at[u, way], line(u, (1, 3)[way]), core)

    def cp_m(ax, d, k):
        src, dst = ((ids_ref, ids), (slots_ref, slots), (gates_ref, gates))[k]
        at = 0 if ax is None else 3 * ax + (4 - d)
        return remote(src, dst.at[at], sm.at[at, k], xm.at[at, k], m if ax is None else shift((ax,), (d,)), other)

    cp_h = remote(resid_ref, resid, sr, xr, m, other)

    def each_m(f):
        for k in range(3):
            f(cp_m(None, 0, k))
            for ax in range(3):
                loop(3, lambda i, ax=ax, k=k: f(cp_m(ax, i + 1, k)))

    def turn_heads(buf, n_blocks, first):
        def step(i):
            for k in range(4):
                buf[first + i * 4 + k] = jnp.swapaxes(buf[first + i * 4 + k], 0, 1)
        loop(n_blocks // 4, step)

    def choose():
        turn[...] = jnp.zeros_like(turn)

        def spread(values, dc):
            for seq in range(n_seq):
                for j in range(top_k):
                    turn[pl.ds((dc * n_seq + seq) * top_k + j, 1), 0:LENGTH] = values[seq, j].astype(f32)

        lane = lax.broadcasted_iota(jnp.int32, (LENGTH, 16 * cap), 1)
        for col in range(3):
            order = ORDERS[col]
            for dc in range(4):
                at = 3 * order[2] + dc if dc else 0
                e, slot = ids[at], slots[at]
                ec = (e >> 4, (e >> 2) & 3, e & 3)
                place = (((m[order[0]] - ec[order[0]]) & 3) * 4 + ((m[order[1]] - ec[order[1]]) & 3)) * cap + slot - flat(shift(order, (0, 0, dc))) * cap
                spread(jnp.where((slot >= 0) & (ec[order[2]] == m[order[2]]), place, -1), dc)
            pos_t = turn[...].T.astype(jnp.int32)
            for dc in range(4):
                spread(gates[3 * order[2] + dc if dc else 0], dc)
            gate_t = turn[...].T
            for dc in range(4):
                for seq in range(n_seq):
                    g = jnp.zeros((LENGTH, 16 * cap), f32)
                    for j in range(top_k):
                        at = (dc * n_seq + seq) * top_k + j
                        g = jnp.where(pos_t[0:LENGTH, at:at + 1] == lane, gate_t[0:LENGTH, at:at + 1], g)
                    for part in range(3):
                        top = g.astype(bf)
                        g_buf[col, dc, pl.ds(part * tokens + seq * LENGTH, LENGTH), :] = top
                        g = g - top.astype(f32)

    def partial(u, dc):
        col, _, wide = UNITS[u]
        rows = rc[u][line(u, dc)[ORDERS[col][2]]].reshape(16 * cap, wide)
        acc = jnp.dot(g_buf[col, dc], rows, preferred_element_type=f32)
        return (acc[:tokens] + acc[tokens:2 * tokens]) + acc[2 * tokens:]

    def send_first(us):
        loop(9, lambda i: [cp_a(u, far(i % 3), far(i // 3)).start() for u in us])
        loop(3, lambda i: [cp_a0(u, far(i)).start() for u in us])
        for u in us:
            cp_own(u).start()
        loop(3, lambda i: [cp_b0(u, far(i)).start() for u in us])

    def pass_on(us):
        def step(i):
            for u in us:
                cp_a(u, far(i % 3), far(i // 3)).wait_recv()
                cp_b(u, far(i % 3), far(i // 3)).start()
        loop(9, step)

    def rows_landed(us):
        for u in us:
            cp_own(u).wait_recv()
        loop(3, lambda i: [cp_a0(u, i + 1).wait_recv() for u in us])
        loop(3, lambda i: [cp_b0(u, i + 1).wait_recv() for u in us])
        loop(9, lambda i: [cp_b(u, far(i // 3), far(i % 3)).wait_recv() for u in us])

    def ring_start(us):
        for u in us:
            s2[u][...] = partial(u, 2)
        for u in us:
            s1[u][...] = partial(u, 1)
            for way in range(2):
                cp_two(u, way).start()
        for u in us:
            s3[u][...] = partial(u, 3)

    def ring_next(us):
        for u in us:
            cp_two(u, 0).wait_recv()
            cp_two(u, 1).wait_recv()
            s1[u][0:half] = s1[u][0:half] + in2[u][0]
            s3[u][half:] = s3[u][half:] + in2[u][1]
        for u in us:
            for way in range(2):
                cp_one(u, way).start()

    def own_sums(us):
        for u in us:
            _, first, wide = UNITS[u]
            own = partial(u, 0)
            cp_one(u, 0).wait_recv()
            cp_one(u, 1).wait_recv()
            y_buf[:, pl.ds(first, wide)] = (resid[:, pl.ds(first, wide)].astype(f32) + ((own + in1[u][...]) + in3[u][...])).astype(bf)

    early, late = (0, 1, 2), (3, 4, 5)
    send_first(early)
    each_m(lambda c: c.start())
    cp_h.start()
    fetches[0].wait()
    turn_heads(tq_ref, 128, 0)
    pass_on(early)
    send_first(late)
    each_m(lambda c: c.wait_recv())
    choose()
    fetches[1].wait()
    turn_heads(tk_ref, 128, 0)
    fetches[2].wait()
    turn_heads(tv_ref, 128, 0)
    rows_landed(early)
    ring_start(early)
    pass_on(late)
    ring_next(early)
    cp_h.wait_recv()
    rows_landed(late)
    ring_start(late)
    own_sums(early)
    ring_next(late)
    own_sums(late)
    fetches[3].wait()

    r = y_buf[...].astype(f32)
    x_buf[...] = (r * lax.rsqrt(jnp.mean(r * r, axis=-1, keepdims=True) + NORM_EPS) * scale_ref[...]).astype(bf)

    t_row = lax.broadcasted_iota(jnp.int32, (tokens, tokens), 0)
    t_col = lax.broadcasted_iota(jnp.int32, (tokens, tokens), 1)
    keep = (t_row >= t_col) & (t_row // LENGTH == t_col // LENGTH)
    for n in range(8):
        x = x_buf[...]
        heads = [jnp.concatenate([t[:, 2 * n].reshape(width, 128), t[:, 2 * n + 1].reshape(width, 128)], axis=1) for t in (tq_ref, tk_ref, tv_ref)]
        q, k, v = [jnp.dot(x, w, preferred_element_type=f32).astype(bf) for w in heads]
        for h in range(2):
            lanes = slice(h * 128, h * 128 + 128)
            s = lax.dot_general(q[:, lanes], k[:, lanes], (((1,), (1,)), ((), ())), preferred_element_type=f32) * 128 ** -0.5
            s = jnp.where(keep, s, -1e30)
            e = jnp.exp(s - jnp.max(s, axis=-1, keepdims=True))
            mixed = jnp.dot(e.astype(bf), v[:, lanes], preferred_element_type=f32)
            a_buf[:, pl.ds((2 * n + h) * 128, 128)] = (mixed / jnp.sum(e, axis=-1, keepdims=True)).astype(bf)

    for n in range(width // 512):
        cols = pl.ds(n * 512, 512)
        proj = jnp.dot(a_buf[...], to_ref[:, cols], preferred_element_type=f32).astype(bf)
        z_ref[:, cols] = (y_buf[:, cols].astype(f32) + proj.astype(f32)).astype(bf)

    cp_h.wait_send()
    each_m(lambda c: c.wait_send())
    for u in range(6):
        cp_own(u).wait_send()
        for way in range(2):
            cp_two(u, way).wait_send()
            cp_one(u, way).wait_send()
    every = range(6)
    loop(9, lambda i: [cp_a(u, 1 + i // 3, 1 + i % 3).wait_send() for u in every])
    loop(9, lambda i: [cp_b(u, 1 + i // 3, 1 + i % 3).wait_send() for u in every])
    loop(3, lambda i: [cp_a0(u, 1 + i).wait_send() for u in every])
    loop(3, lambda i: [cp_b0(u, 1 + i).wait_send() for u in every])


def run_stage(o, ids, slots, gates, resid, scale, wq, wk, wv, wo):
    bf, f32 = jnp.bfloat16, jnp.float32
    cap, width = o.shape[3:]
    tokens = resid.shape[0]
    dma, buf = pltpu.SemaphoreType.DMA, pltpu.VMEM
    hbm, vmem = pl.BlockSpec(memory_space=pl.ANY), pl.BlockSpec(memory_space=pltpu.VMEM)
    sums = [buf((tokens, w), f32) for _, _, w in UNITS]
    pairs = [buf((2, tokens // 2, w), f32) for _, _, w in UNITS]
    sems = [dma((6, 3, 4)), dma((6, 3, 4)), dma((6,)), dma((6,)), dma((6, 4, 3)), dma((6, 4, 3)), dma((6, 2)), dma((6, 2)), dma((6, 2)), dma((6, 2)),
            dma((10, 3)), dma((10, 3)), dma(()), dma(()), dma((4,))]
    return pl.pallas_call(
        stage_kernel,
        out_shape=jax.ShapeDtypeStruct((tokens, width), bf),
        in_specs=[hbm] * 5 + [vmem] + [hbm] * 4,
        out_specs=vmem,
        scratch_shapes=[buf(wq.shape, bf)] * 3 + [buf(wo.shape, bf)]
        + [buf((10,) + ids.shape, ids.dtype), buf((10,) + slots.shape, slots.dtype), buf((10,) + gates.shape, gates.dtype), buf(resid.shape, bf)]
        + [buf((3, 4, 3 * tokens, 16 * cap), bf)] + [buf((tokens, width), bf)] * 3 + [buf((128, 128), f32)]
        + [[buf((3, 3, 4, cap, w), bf) for _, _, w in UNITS], [buf((4, 16, cap, w), bf) for _, _, w in UNITS]]
        + [sums, sums, sums, sums, pairs, sums] + [sems],
        compiler_params=pltpu.CompilerParams(collective_id=0, has_side_effects=True, vmem_limit_bytes=63 * 2**20),
    )(o, ids, slots, gates, resid, scale, wq, wk, wv, wo)


def solution(mesh):
    token_spec = P(('data', 'pp'), 'ep', None, None)
    weight_spec = P('pp', None, None, None)

    def body(expert_out, expert_ids, slot_ids, gate_vals, residual, norm_scale, w_query, w_key, w_value, w_out):
        width = expert_out.shape[-1]
        cap = expert_out.shape[2] // 64
        seqs, length, top_k = expert_ids.shape[1:]
        ids, slots, gates = [jnp.transpose(a, (1, 3, 0, 2)) for a in (expert_ids, slot_ids, gate_vals)]
        result = run_stage(expert_out[0, 0].reshape(4, 4, 4, cap, width), ids, slots, gates, residual[0].reshape(-1, width),
                           norm_scale, *[w[0].reshape(width // 16, 16, 16, 128) for w in (w_query, w_key, w_value)], w_out[0].reshape(width, width))
        return result.reshape(residual.shape)

    return jax.shard_map(body, mesh=mesh, in_specs=(token_spec, token_spec, token_spec, token_spec, token_spec, P('pp', None), weight_spec, weight_spec, weight_spec, weight_spec), out_specs=token_spec, check_vma=False)
```

```python
import jax
import jax.numpy as jnp
from jax import lax
from jax.experimental import pallas as pl
from jax.experimental.pallas import tpu as pltpu
from jax.sharding import PartitionSpec as P

NORM_EPS = 1e-6
MESH = pl.DeviceIdType.MESH
ORDERS = ((2, 1, 0), (1, 0, 2), (0, 2, 1))
UNITS = ((0, 0, 512), (1, 768, 384), (2, 1408, 384), (0, 512, 256), (1, 1152, 256), (2, 1792, 256))
LENGTH = 48


def stage_kernel(o_ref, ids_ref, slots_ref, gates_ref, resid_ref, scale_ref, wq_ref, wk_ref, wv_ref, wo_ref, z_ref,
                 tq_ref, tk_ref, tv_ref, to_ref, scale, ids, slots, gates, resid, own_buf, g_buf, y_buf, x_buf, a_buf, turn,
                 ra, rc, s1, s2, s3, in1, in2, in3, sems):
    f32, bf = jnp.float32, jnp.bfloat16
    me = lax.axis_index('ep')
    core = lax.axis_index('pp')
    other = 1 - core
    m = (me // 16, (me // 4) % 4, me % 4)
    tokens, width = resid_ref.shape
    cap = o_ref.shape[3]
    n_seq, top_k = ids_ref.shape[:2]
    half = tokens // 2
    sa, xa, so, xo, sb, xb, s_two, x_two, s_one, x_one, sm, xm, sr, xr, sw = sems

    def shift(order, deltas):
        c = list(m)
        for ax, d in zip(order, deltas):
            c[ax] = (c[ax] + d) % 4
        return c

    def flat(c):
        return c[0] * 16 + c[1] * 4 + c[2]

    def dev(c, core_id):
        return {'pp': core_id, 'ep': flat(c)}

    def far(i):
        return 1 + (2 * i) % 3

    def loop(n, step):
        lax.fori_loop(0, n, lambda i, _: (step(i), 0)[1], 0)

    fetches = [pltpu.make_async_copy(w, t, sw.at[i]) for i, (w, t) in enumerate(((wq_ref, tq_ref), (wk_ref, tk_ref), (wv_ref, tv_ref), (wo_ref, to_ref), (scale_ref, scale)))]
    for fetch in fetches:
        fetch.start()

    barrier = pltpu.get_barrier_semaphore()

    def greet(i):
        for ax in range(3):
            for cid in (core, other):
                pl.semaphore_signal(barrier, inc=1, device_id=dev(shift((ax,), (i + 1,)), cid), device_id_type=MESH)

    loop(3, greet)
    pl.semaphore_signal(barrier, inc=1, device_id=dev(m, other), device_id_type=MESH)
    pl.semaphore_wait(barrier, 19)

    def osrc(u, a, b):
        col, first, wide = UNITS[u]
        order = ORDERS[col]
        idx = [slice(None)] * 3
        idx[order[0]] = a
        idx[order[1]] = b
        return o_ref.at[idx[0], idx[1], idx[2], :, pl.ds(first, wide)]

    def remote(src, dst, send, recv, c, core_id):
        return pltpu.make_async_remote_copy(src_ref=src, dst_ref=dst, send_sem=send, recv_sem=recv, device_id=dev(c, core_id), device_id_type=MESH)

    def cp_a(u, da, db):
        order = ORDERS[UNITS[u][0]]
        c = shift(order, (da, db, 0))
        return remote(osrc(u, c[order[0]], c[order[1]]), ra[u].at[da - 1, db - 1], sa.at[u, da - 1, db], xa.at[u, da - 1, db],
                      shift(order, (da, 0, 0)), other)

    def cp_a0(u, da):
        order = ORDERS[UNITS[u][0]]
        c = shift(order, (da, 0, 0))
        return remote(osrc(u, c[order[0]], c[order[1]]), rc[u].at[:, da * 4], sa.at[u, da - 1, 0], xa.at[u, da - 1, 0], c, other)

    def cp_own(u):
        order = ORDERS[UNITS[u][0]]
        return remote(osrc(u, m[order[0]], m[order[1]]), rc[u].at[:, 0], so.at[u], xo.at[u], m, other)

    def cp_b(u, da, db):
        return remote(ra[u].at[da - 1, db - 1], rc[u].at[:, da * 4 + db], sb.at[u, da, db - 1], xb.at[u, da, db - 1],
                      shift(ORDERS[UNITS[u][0]], (0, db, 0)), core)

    def cp_b0(u, db):
        order = ORDERS[UNITS[u][0]]
        c = shift(order, (0, db, 0))
        return remote(osrc(u, c[order[0]], c[order[1]]), rc[u].at[:, db], sb.at[u, 0, db - 1], xb.at[u, 0, db - 1], c, other)

    def line(u, d):
        return shift(ORDERS[UNITS[u][0]], (0, 0, d))

    def cp_two(u, way):
        return remote(s2[u].at[pl.ds(way * half, half)], in2[u].at[way], s_two.at[u, way], x_two.at[u, way], line(u, (1, 3)[way]), core)

    def cp_one(u, way):
        return remote((s1, s3)[way][u], (in1, in3)[way][u], s_one.at[u, way], x_one.at[u, way], line(u, (1, 3)[way]), core)

    def cp_m(ax, d, k):
        src, dst = ((ids_ref, ids), (slots_ref, slots), (gates_ref, gates))[k]
        at = 0 if ax is None else 3 * ax + (4 - d)
        return remote(src, dst.at[at], sm.at[at, k], xm.at[at, k], m if ax is None else shift((ax,), (d,)), other)

    cp_h = remote(resid_ref, resid, sr, xr, m, other)

    def each_m(f):
        for k in range(3):
            f(cp_m(None, 0, k))
            for ax in range(3):
                loop(3, lambda i, ax=ax, k=k: f(cp_m(ax, i + 1, k)))

    def turn_heads(buf, n_blocks, first):
        def step(i):
            for k in range(4):
                buf[first + i * 4 + k] = jnp.swapaxes(buf[first + i * 4 + k], 0, 1)
        loop(n_blocks // 4, step)

    def choose():
        turn[...] = jnp.zeros_like(turn)

        def spread(values, dc):
            for seq in range(n_seq):
                for j in range(top_k):
                    turn[pl.ds((dc * n_seq + seq) * top_k + j, 1), 0:LENGTH] = values[seq, j].astype(f32)

        lane = lax.broadcasted_iota(jnp.int32, (LENGTH, 16 * cap), 1)
        for col in range(3):
            order = ORDERS[col]
            for dc in range(4):
                at = 3 * order[2] + dc if dc else 0
                e, slot = ids[at], slots[at]
                ec = (e >> 4, (e >> 2) & 3, e & 3)
                place = (((m[order[0]] - ec[order[0]]) & 3) * 4 + ((m[order[1]] - ec[order[1]]) & 3)) * cap + slot - flat(shift(order, (0, 0, dc))) * cap
                spread(jnp.where((slot >= 0) & (ec[order[2]] == m[order[2]]), place, -1), dc)
            pos_t = turn[...].T.astype(jnp.int32)
            for dc in range(4):
                spread(gates[3 * order[2] + dc if dc else 0], dc)
            gate_t = turn[...].T
            for dc in range(4):
                for seq in range(n_seq):
                    g = jnp.zeros((LENGTH, 16 * cap), f32)
                    for j in range(top_k):
                        at = (dc * n_seq + seq) * top_k + j
                        g = jnp.where(pos_t[0:LENGTH, at:at + 1] == lane, gate_t[0:LENGTH, at:at + 1], g)
                    for part in range(3):
                        top = g.astype(bf)
                        g_buf[col, dc, pl.ds(part * tokens + seq * LENGTH, LENGTH), :] = top
                        g = g - top.astype(f32)

    def partial(u, dc):
        col, _, wide = UNITS[u]
        rows = rc[u][line(u, dc)[ORDERS[col][2]]].reshape(16 * cap, wide)
        acc = jnp.dot(g_buf[col, dc], rows, preferred_element_type=f32)
        return (acc[:tokens] + acc[tokens:2 * tokens]) + acc[2 * tokens:]

    def send_first(us):
        loop(9, lambda i: [cp_a(u, far(i % 3), far(i // 3)).start() for u in us])
        loop(3, lambda i: [cp_a0(u, far(i)).start() for u in us])
        for u in us:
            cp_own(u).start()
        loop(3, lambda i: [cp_b0(u, far(i)).start() for u in us])

    def pass_on(us):
        def step(i):
            for u in us:
                cp_a(u, far(i % 3), far(i // 3)).wait_recv()
                cp_b(u, far(i % 3), far(i // 3)).start()
        loop(9, step)

    def rows_landed(us):
        for u in us:
            cp_own(u).wait_recv()
        loop(3, lambda i: [cp_a0(u, i + 1).wait_recv() for u in us])
        loop(3, lambda i: [cp_b0(u, i + 1).wait_recv() for u in us])
        loop(9, lambda i: [cp_b(u, far(i // 3), far(i % 3)).wait_recv() for u in us])

    def ring_start(us):
        def send(u):
            for way in range(2):
                cp_two(u, way).start()
        for k, u in enumerate(us):
            s2[u][...] = partial(u, 2)
            if k:
                send(us[k - 1])
        for k, u in enumerate(us):
            s1[u][...] = partial(u, 1)
            if k == 0:
                send(us[-1])
        for u in us:
            s3[u][...] = partial(u, 3)
        for u in us:
            cols = pl.ds(UNITS[u][1], UNITS[u][2])
            own_buf[:, cols] = resid[:, cols].astype(f32) + partial(u, 0)

    def ring_next(us):
        for u in us:
            cp_two(u, 0).wait_recv()
            cp_two(u, 1).wait_recv()
            s1[u][0:half] = s1[u][0:half] + in2[u][0]
            s3[u][half:] = s3[u][half:] + in2[u][1]
        for u in us:
            for way in range(2):
                cp_one(u, way).start()

    def own_sums(us):
        for u in us:
            _, first, wide = UNITS[u]
            cp_one(u, 0).wait_recv()
            cp_one(u, 1).wait_recv()
            y_buf[:, pl.ds(first, wide)] = ((own_buf[:, pl.ds(first, wide)] + in1[u][...]) + in3[u][...]).astype(bf)

    early, late = (0, 1, 2), (3, 4, 5)
    send_first(early)
    each_m(lambda c: c.start())
    cp_h.start()
    fetches[0].wait()
    turn_heads(tq_ref, 128, 0)
    pass_on(early)
    send_first(late)
    each_m(lambda c: c.wait_recv())
    choose()
    fetches[1].wait()
    turn_heads(tk_ref, 128, 0)
    fetches[2].wait()
    turn_heads(tv_ref, 128, 0)
    cp_h.wait_recv()
    rows_landed(early)
    ring_start(early)
    pass_on(late)
    ring_next(early)
    rows_landed(late)
    ring_start(late)
    own_sums(early)
    ring_next(late)
    own_sums(late)
    fetches[3].wait()
    fetches[4].wait()

    r = y_buf[...].astype(f32)
    x_buf[...] = (r * lax.rsqrt(jnp.mean(r * r, axis=-1, keepdims=True) + NORM_EPS) * scale[...]).astype(bf)

    t_row = lax.broadcasted_iota(jnp.int32, (tokens, tokens), 0)
    t_col = lax.broadcasted_iota(jnp.int32, (tokens, tokens), 1)
    keep = (t_row >= t_col) & (t_row // LENGTH == t_col // LENGTH)
    def project(n):
        x = x_buf[...]
        heads = [jnp.concatenate([t[:, 2 * n].reshape(width, 128), t[:, 2 * n + 1].reshape(width, 128)], axis=1) for t in (tq_ref, tk_ref, tv_ref)]
        return [jnp.dot(x, w, preferred_element_type=f32).astype(bf) for w in heads]

    def mix(n, q, k, v):
        for h in range(2):
            lanes = slice(h * 128, h * 128 + 128)
            s = lax.dot_general(q[:, lanes], k[:, lanes], (((1,), (1,)), ((), ())), preferred_element_type=f32) * 128 ** -0.5
            s = jnp.where(keep, s, -1e30)
            e = jnp.exp(s - jnp.max(s, axis=-1, keepdims=True))
            mixed = jnp.dot(e.astype(bf), v[:, lanes], preferred_element_type=f32)
            a_buf[:, pl.ds((2 * n + h) * 128, 128)] = (mixed / jnp.sum(e, axis=-1, keepdims=True)).astype(bf)

    held = project(0)
    for n in range(8):
        ahead = project(n + 1) if n < 7 else None
        mix(n, *held)
        held = ahead

    for n in range(width // 512):
        cols = pl.ds(n * 512, 512)
        proj = jnp.dot(a_buf[...], to_ref[:, cols], preferred_element_type=f32).astype(bf)
        z_ref[:, cols] = (y_buf[:, cols].astype(f32) + proj.astype(f32)).astype(bf)

    cp_h.wait_send()
    each_m(lambda c: c.wait_send())
    for u in range(6):
        cp_own(u).wait_send()
        for way in range(2):
            cp_two(u, way).wait_send()
            cp_one(u, way).wait_send()
    every = range(6)
    loop(9, lambda i: [cp_a(u, 1 + i // 3, 1 + i % 3).wait_send() for u in every])
    loop(9, lambda i: [cp_b(u, 1 + i // 3, 1 + i % 3).wait_send() for u in every])
    loop(3, lambda i: [cp_a0(u, 1 + i).wait_send() for u in every])
    loop(3, lambda i: [cp_b0(u, 1 + i).wait_send() for u in every])


def run_stage(o, ids, slots, gates, resid, scale, wq, wk, wv, wo):
    bf, f32 = jnp.bfloat16, jnp.float32
    cap, width = o.shape[3:]
    tokens = resid.shape[0]
    dma, buf = pltpu.SemaphoreType.DMA, pltpu.VMEM
    hbm, vmem = pl.BlockSpec(memory_space=pl.ANY), pl.BlockSpec(memory_space=pltpu.VMEM)
    sums = [buf((tokens, w), f32) for _, _, w in UNITS]
    pairs = [buf((2, tokens // 2, w), f32) for _, _, w in UNITS]
    sems = [dma((6, 3, 4)), dma((6, 3, 4)), dma((6,)), dma((6,)), dma((6, 4, 3)), dma((6, 4, 3)), dma((6, 2)), dma((6, 2)), dma((6, 2)), dma((6, 2)),
            dma((10, 3)), dma((10, 3)), dma(()), dma(()), dma((5,))]
    return pl.pallas_call(
        stage_kernel,
        out_shape=pltpu.VMEM((tokens, width), bf),
        in_specs=[hbm] * 10,
        out_specs=vmem,
        scratch_shapes=[buf(wq.shape, bf)] * 3 + [buf(wo.shape, bf), buf(scale.shape, f32)]
        + [buf((10,) + ids.shape, ids.dtype), buf((10,) + slots.shape, slots.dtype), buf((10,) + gates.shape, gates.dtype), buf(resid.shape, bf), buf(resid.shape, f32)]
        + [buf((3, 4, 3 * tokens, 16 * cap), bf)] + [buf((tokens, width), bf)] * 3 + [buf((128, 128), f32)]
        + [[buf((3, 3, 4, cap, w), bf) for _, _, w in UNITS], [buf((4, 16, cap, w), bf) for _, _, w in UNITS]]
        + [sums, sums, sums, sums, pairs, sums] + [sems],
        compiler_params=pltpu.CompilerParams(collective_id=0, has_side_effects=True, vmem_limit_bytes=63 * 2**20),
    )(o, ids, slots, gates, resid, scale, wq, wk, wv, wo)


def solution(mesh):
    token_spec = P(('data', 'pp'), 'ep', None, None)
    weight_spec = P('pp', None, None, None)

    def body(expert_out, expert_ids, slot_ids, gate_vals, residual, norm_scale, w_query, w_key, w_value, w_out):
        width = expert_out.shape[-1]
        cap = expert_out.shape[2] // 64
        seqs, length, top_k = expert_ids.shape[1:]
        ids, slots, gates = [jnp.transpose(a, (1, 3, 0, 2)) for a in (expert_ids, slot_ids, gate_vals)]
        result = run_stage(expert_out[0, 0].reshape(4, 4, 4, cap, width), ids, slots, gates, residual[0].reshape(-1, width),
                           norm_scale, *[w[0].reshape(width // 16, 16, 16, 128) for w in (w_query, w_key, w_value)], w_out[0].reshape(width, width))
        return result.reshape(residual.shape)

    return jax.shard_map(body, mesh=mesh, in_specs=(token_spec, token_spec, token_spec, token_spec, token_spec, P('pp', None), weight_spec, weight_spec, weight_spec, weight_spec), out_specs=token_spec, check_vma=False)
```

```python
import jax
import jax.numpy as jnp
from jax import lax
from jax.experimental import pallas as pl
from jax.experimental.pallas import tpu as pltpu
from jax.sharding import PartitionSpec as P

NORM_EPS = 1e-6
MESH = pl.DeviceIdType.MESH
ORDERS = ((2, 1, 0), (1, 0, 2), (0, 2, 1))
UNITS = ((0, 0, 512), (1, 768, 384), (2, 1408, 384), (0, 512, 256), (1, 1152, 256), (2, 1792, 256))
LENGTH = 48


def stage_kernel(o_ref, ids_ref, slots_ref, gates_ref, resid_ref, scale_ref, wq_ref, wk_ref, wv_ref, wo_ref, z_ref,
                 tq_ref, tk_ref, tv_ref, to_ref, scale, ids, slots, gates, resid, own_buf, g_buf, y_buf, x_buf, a_buf, turn,
                 ra, rc, s1, s2, s3, in1, in2, in3, sems):
    f32, bf = jnp.float32, jnp.bfloat16
    me = lax.axis_index('ep')
    core = lax.axis_index('pp')
    other = 1 - core
    m = (me // 16, (me // 4) % 4, me % 4)
    tokens, width = resid_ref.shape
    cap = o_ref.shape[3]
    n_seq, top_k = ids_ref.shape[:2]
    half = tokens // 2
    sa, xa, so, xo, sb, xb, s_two, x_two, s_one, x_one, sm, xm, sr, xr, sw = sems

    def shift(order, deltas):
        c = list(m)
        for ax, d in zip(order, deltas):
            c[ax] = (c[ax] + d) % 4
        return c

    def flat(c):
        return c[0] * 16 + c[1] * 4 + c[2]

    def dev(c, core_id):
        return {'pp': core_id, 'ep': flat(c)}

    def far(i):
        return 1 + (2 * i) % 3

    def loop(n, step):
        lax.fori_loop(0, n, lambda i, _: (step(i), 0)[1], 0)

    fetches = [pltpu.make_async_copy(w, t, sw.at[i]) for i, (w, t) in enumerate(((wq_ref, tq_ref), (wk_ref, tk_ref), (wv_ref, tv_ref), (wo_ref, to_ref), (scale_ref, scale)))]
    for fetch in fetches:
        fetch.start()

    barrier = pltpu.get_barrier_semaphore()

    def greet(i):
        for ax in range(3):
            for cid in (core, other):
                pl.semaphore_signal(barrier, inc=1, device_id=dev(shift((ax,), (i + 1,)), cid), device_id_type=MESH)

    loop(3, greet)
    pl.semaphore_signal(barrier, inc=1, device_id=dev(m, other), device_id_type=MESH)
    pl.semaphore_wait(barrier, 19)

    def osrc(u, a, b):
        col, first, wide = UNITS[u]
        order = ORDERS[col]
        idx = [slice(None)] * 3
        idx[order[0]] = a
        idx[order[1]] = b
        return o_ref.at[idx[0], idx[1], idx[2], :, pl.ds(first, wide)]

    def remote(src, dst, send, recv, c, core_id):
        return pltpu.make_async_remote_copy(src_ref=src, dst_ref=dst, send_sem=send, recv_sem=recv, device_id=dev(c, core_id), device_id_type=MESH)

    def cp_a(u, da, db):
        order = ORDERS[UNITS[u][0]]
        c = shift(order, (da, db, 0))
        return remote(osrc(u, c[order[0]], c[order[1]]), ra[u].at[da - 1, db - 1], sa.at[u, da - 1, db], xa.at[u, da - 1, db],
                      shift(order, (da, 0, 0)), other)

    def cp_a0(u, da):
        order = ORDERS[UNITS[u][0]]
        c = shift(order, (da, 0, 0))
        return remote(osrc(u, c[order[0]], c[order[1]]), rc[u].at[:, da * 4], sa.at[u, da - 1, 0], xa.at[u, da - 1, 0], c, other)

    def cp_own(u):
        order = ORDERS[UNITS[u][0]]
        return remote(osrc(u, m[order[0]], m[order[1]]), rc[u].at[:, 0], so.at[u], xo.at[u], m, other)

    def cp_b(u, da, db):
        return remote(ra[u].at[da - 1, db - 1], rc[u].at[:, da * 4 + db], sb.at[u, da, db - 1], xb.at[u, da, db - 1],
                      shift(ORDERS[UNITS[u][0]], (0, db, 0)), core)

    def cp_b0(u, db):
        order = ORDERS[UNITS[u][0]]
        c = shift(order, (0, db, 0))
        return remote(osrc(u, c[order[0]], c[order[1]]), rc[u].at[:, db], sb.at[u, 0, db - 1], xb.at[u, 0, db - 1], c, other)

    def line(u, d):
        return shift(ORDERS[UNITS[u][0]], (0, 0, d))

    def cp_two(u, way):
        return remote(s2[u].at[pl.ds(way * half, half)], in2[u].at[way], s_two.at[u, way], x_two.at[u, way], line(u, (1, 3)[way]), core)

    def cp_one(u, way):
        return remote((s1, s3)[way][u], (in1, in3)[way][u], s_one.at[u, way], x_one.at[u, way], line(u, (1, 3)[way]), core)

    def cp_m(ax, d, k):
        src, dst = ((ids_ref, ids), (slots_ref, slots), (gates_ref, gates))[k]
        at = 0 if ax is None else 3 * ax + (4 - d)
        return remote(src, dst.at[at], sm.at[at, k], xm.at[at, k], m if ax is None else shift((ax,), (d,)), other)

    cp_h = remote(resid_ref, resid, sr, xr, m, other)

    def each_m(f):
        for k in range(3):
            f(cp_m(None, 0, k))
            for ax in range(3):
                loop(3, lambda i, ax=ax, k=k: f(cp_m(ax, i + 1, k)))

    def turn_heads(buf, n_blocks, first):
        def step(i):
            for k in range(4):
                buf[first + i * 4 + k] = jnp.swapaxes(buf[first + i * 4 + k], 0, 1)
        loop(n_blocks // 4, step)

    def choose():
        turn[...] = jnp.zeros_like(turn)

        def spread(values, dc):
            for seq in range(n_seq):
                for j in range(top_k):
                    turn[pl.ds((dc * n_seq + seq) * top_k + j, 1), 0:LENGTH] = values[seq, j].astype(f32)

        lane = lax.broadcasted_iota(jnp.int32, (LENGTH, 16 * cap), 1)
        for col in range(3):
            order = ORDERS[col]
            for dc in range(4):
                at = 3 * order[2] + dc if dc else 0
                e, slot = ids[at], slots[at]
                ec = (e >> 4, (e >> 2) & 3, e & 3)
                place = (((m[order[0]] - ec[order[0]]) & 3) * 4 + ((m[order[1]] - ec[order[1]]) & 3)) * cap + slot - flat(shift(order, (0, 0, dc))) * cap
                spread(jnp.where((slot >= 0) & (ec[order[2]] == m[order[2]]), place, -1), dc)
            pos_t = turn[...].T.astype(jnp.int32)
            for dc in range(4):
                spread(gates[3 * order[2] + dc if dc else 0], dc)
            gate_t = turn[...].T
            for dc in range(4):
                for seq in range(n_seq):
                    g = jnp.zeros((LENGTH, 16 * cap), f32)
                    for j in range(top_k):
                        at = (dc * n_seq + seq) * top_k + j
                        g = jnp.where(pos_t[0:LENGTH, at:at + 1] == lane, gate_t[0:LENGTH, at:at + 1], g)
                    for part in range(3):
                        top = g.astype(bf)
                        g_buf[col, dc, pl.ds(part * tokens + seq * LENGTH, LENGTH), :] = top
                        g = g - top.astype(f32)

    def partial(u, dc):
        col, _, wide = UNITS[u]
        rows = rc[u][line(u, dc)[ORDERS[col][2]]].reshape(16 * cap, wide)
        acc = jnp.dot(g_buf[col, dc], rows, preferred_element_type=f32)
        return (acc[:tokens] + acc[tokens:2 * tokens]) + acc[2 * tokens:]

    def send_first(us):
        loop(9, lambda i: [cp_a(u, far(i % 3), far(i // 3)).start() for u in us])
        loop(3, lambda i: [cp_a0(u, far(i)).start() for u in us])
        for u in us:
            cp_own(u).start()
        loop(3, lambda i: [cp_b0(u, far(i)).start() for u in us])

    def pass_on(us):
        def step(i):
            for u in us:
                cp_a(u, far(i % 3), far(i // 3)).wait_recv()
                cp_b(u, far(i % 3), far(i // 3)).start()
        loop(9, step)

    def rows_landed(us):
        for u in us:
            cp_own(u).wait_recv()
        loop(3, lambda i: [cp_a0(u, i + 1).wait_recv() for u in us])
        loop(3, lambda i: [cp_b0(u, i + 1).wait_recv() for u in us])
        loop(9, lambda i: [cp_b(u, far(i // 3), far(i % 3)).wait_recv() for u in us])

    def ring_start(us):
        def send(u):
            for way in range(2):
                cp_two(u, way).start()
        for k, u in enumerate(us):
            s2[u][...] = partial(u, 2)
            if k:
                send(us[k - 1])
        for k, u in enumerate(us):
            s1[u][...] = partial(u, 1)
            if k == 0:
                send(us[-1])
        for u in us:
            s3[u][...] = partial(u, 3)
        for u in us:
            cols = pl.ds(UNITS[u][1], UNITS[u][2])
            own_buf[:, cols] = resid[:, cols].astype(f32) + partial(u, 0)

    def ring_next(us):
        for u in us:
            cp_two(u, 0).wait_recv()
            cp_two(u, 1).wait_recv()
            s1[u][0:half] = s1[u][0:half] + in2[u][0]
            s3[u][half:] = s3[u][half:] + in2[u][1]
        for u in us:
            for way in range(2):
                cp_one(u, way).start()

    def own_sums(us):
        for u in us:
            _, first, wide = UNITS[u]
            cp_one(u, 0).wait_recv()
            cp_one(u, 1).wait_recv()
            y_buf[:, pl.ds(first, wide)] = ((own_buf[:, pl.ds(first, wide)] + in1[u][...]) + in3[u][...]).astype(bf)

    def first_left(us):
        loop(9, lambda i: [cp_a(u, 1 + i // 3, 1 + i % 3).wait_send() for u in us])
        loop(3, lambda i: [cp_a0(u, 1 + i).wait_send() for u in us])
        loop(3, lambda i: [cp_b0(u, 1 + i).wait_send() for u in us])
        for u in us:
            cp_own(u).wait_send()

    def second_left(us):
        loop(9, lambda i: [cp_b(u, 1 + i // 3, 1 + i % 3).wait_send() for u in us])

    def ring_left(us):
        for u in us:
            for way in range(2):
                cp_two(u, way).wait_send()
                cp_one(u, way).wait_send()

    early, late = (0, 1, 2), (3, 4, 5)
    send_first(early)
    each_m(lambda c: c.start())
    cp_h.start()
    fetches[0].wait()
    turn_heads(tq_ref, 128, 0)
    pass_on(early)
    send_first(late)
    each_m(lambda c: c.wait_recv())
    choose()
    fetches[1].wait()
    turn_heads(tk_ref, 128, 0)
    fetches[2].wait()
    turn_heads(tv_ref, 128, 0)
    cp_h.wait_recv()
    rows_landed(early)
    ring_start(early)
    pass_on(late)
    ring_next(early)
    cp_h.wait_send()
    each_m(lambda c: c.wait_send())
    first_left(early + late)
    second_left(early)
    rows_landed(late)
    ring_start(late)
    own_sums(early)
    ring_next(late)
    second_left(late)
    ring_left(early)
    own_sums(late)
    fetches[3].wait()
    fetches[4].wait()

    r = y_buf[...].astype(f32)
    x_buf[...] = (r * lax.rsqrt(jnp.mean(r * r, axis=-1, keepdims=True) + NORM_EPS) * scale[...]).astype(bf)

    t_row = lax.broadcasted_iota(jnp.int32, (tokens, tokens), 0)
    t_col = lax.broadcasted_iota(jnp.int32, (tokens, tokens), 1)
    keep = (t_row >= t_col) & (t_row // LENGTH == t_col // LENGTH)
    def project(n):
        x = x_buf[...]
        heads = [jnp.concatenate([t[:, 2 * n].reshape(width, 128), t[:, 2 * n + 1].reshape(width, 128)], axis=1) for t in (tq_ref, tk_ref, tv_ref)]
        return [jnp.dot(x, w, preferred_element_type=f32).astype(bf) for w in heads]

    def weigh(q, k):
        out = []
        for h in range(2):
            lanes = slice(h * 128, h * 128 + 128)
            s = lax.dot_general(q[:, lanes], k[:, lanes], (((1,), (1,)), ((), ())), preferred_element_type=f32) * 128 ** -0.5
            s = jnp.where(keep, s, -1e30)
            e = jnp.exp(s - jnp.max(s, axis=-1, keepdims=True))
            out.append((e.astype(bf), jnp.sum(e, axis=-1, keepdims=True)))
        return out

    def mix(n, weights, v):
        for h, (e, total) in enumerate(weights):
            mixed = jnp.dot(e, v[:, h * 128:h * 128 + 128], preferred_element_type=f32)
            a_buf[:, pl.ds((2 * n + h) * 128, 128)] = (mixed / total).astype(bf)

    q, k, v = project(0)
    held = None
    for n in range(8):
        ahead = project(n + 1) if n < 7 else None
        weights = weigh(q, k)
        if held is not None:
            mix(n - 1, *held)
        held = (weights, v)
        if ahead is not None:
            q, k, v = ahead
    mix(7, *held)

    for n in range(width // 512):
        cols = pl.ds(n * 512, 512)
        proj = jnp.dot(a_buf[...], to_ref[:, cols], preferred_element_type=f32).astype(bf)
        z_ref[:, cols] = (y_buf[:, cols].astype(f32) + proj.astype(f32)).astype(bf)

    ring_left(late)


def run_stage(o, ids, slots, gates, resid, scale, wq, wk, wv, wo):
    bf, f32 = jnp.bfloat16, jnp.float32
    cap, width = o.shape[3:]
    tokens = resid.shape[0]
    dma, buf = pltpu.SemaphoreType.DMA, pltpu.VMEM
    hbm, vmem = pl.BlockSpec(memory_space=pl.ANY), pl.BlockSpec(memory_space=pltpu.VMEM)
    sums = [buf((tokens, w), f32) for _, _, w in UNITS]
    pairs = [buf((2, tokens // 2, w), f32) for _, _, w in UNITS]
    sems = [dma((6, 3, 4)), dma((6, 3, 4)), dma((6,)), dma((6,)), dma((6, 4, 3)), dma((6, 4, 3)), dma((6, 2)), dma((6, 2)), dma((6, 2)), dma((6, 2)),
            dma((10, 3)), dma((10, 3)), dma(()), dma(()), dma((5,))]
    return pl.pallas_call(
        stage_kernel,
        out_shape=pltpu.VMEM((tokens, width), bf),
        in_specs=[hbm] * 10,
        out_specs=vmem,
        scratch_shapes=[buf(wq.shape, bf)] * 3 + [buf(wo.shape, bf), buf(scale.shape, f32)]
        + [buf((10,) + ids.shape, ids.dtype), buf((10,) + slots.shape, slots.dtype), buf((10,) + gates.shape, gates.dtype), buf(resid.shape, bf), buf(resid.shape, f32)]
        + [buf((3, 4, 3 * tokens, 16 * cap), bf)] + [buf((tokens, width), bf)] * 3 + [buf((128, 128), f32)]
        + [[buf((3, 3, 4, cap, w), bf) for _, _, w in UNITS], [buf((4, 16, cap, w), bf) for _, _, w in UNITS]]
        + [sums, sums, sums, sums, pairs, sums] + [sems],
        compiler_params=pltpu.CompilerParams(collective_id=0, has_side_effects=True, vmem_limit_bytes=63 * 2**20),
    )(o, ids, slots, gates, resid, scale, wq, wk, wv, wo)


def solution(mesh):
    token_spec = P(('data', 'pp'), 'ep', None, None)
    weight_spec = P('pp', None, None, None)

    def body(expert_out, expert_ids, slot_ids, gate_vals, residual, norm_scale, w_query, w_key, w_value, w_out):
        width = expert_out.shape[-1]
        cap = expert_out.shape[2] // 64
        seqs, length, top_k = expert_ids.shape[1:]
        ids, slots, gates = [jnp.transpose(a, (1, 3, 0, 2)) for a in (expert_ids, slot_ids, gate_vals)]
        result = run_stage(expert_out[0, 0].reshape(4, 4, 4, cap, width), ids, slots, gates, residual[0].reshape(-1, width),
                           norm_scale, *[w[0].reshape(width // 16, 16, 16, 128) for w in (w_query, w_key, w_value)], w_out[0].reshape(width, width))
        return result.reshape(residual.shape)

    return jax.shard_map(body, mesh=mesh, in_specs=(token_spec, token_spec, token_spec, token_spec, token_spec, P('pp', None), weight_spec, weight_spec, weight_spec, weight_spec), out_specs=token_spec, check_vma=False)
```

```python
import jax
import jax.numpy as jnp
from jax import lax
from jax.experimental import pallas as pl
from jax.experimental.pallas import tpu as pltpu
from jax.sharding import PartitionSpec as P

NORM_EPS = 1e-6
MESH = pl.DeviceIdType.MESH
ORDERS = ((2, 1, 0), (1, 0, 2), (0, 2, 1))
UNITS = ((0, 0, 512), (1, 768, 384), (2, 1408, 384), (0, 512, 256), (1, 1152, 256), (2, 1792, 256))
LENGTH = 48


def stage_kernel(o_ref, ids_ref, slots_ref, gates_ref, resid_ref, scale_ref, wq_ref, wk_ref, wv_ref, wo_ref, z_ref,
                 tq_ref, tk_ref, tv_ref, to_ref, scale, ids, slots, gates, resid, own_buf, g_buf, y_buf, x_buf, a_buf, turn,
                 ra, rc, s1, s2, s3, in1, in2, in3, sems):
    f32, bf = jnp.float32, jnp.bfloat16
    me = lax.axis_index('ep')
    core = lax.axis_index('pp')
    other = 1 - core
    m = (me // 16, (me // 4) % 4, me % 4)
    tokens, width = resid_ref.shape
    cap = o_ref.shape[3]
    n_seq, top_k = ids_ref.shape[:2]
    half = tokens // 2
    sa, xa, so, xo, sb, xb, s_two, x_two, s_one, x_one, sm, xm, sr, xr, sw = sems

    def shift(order, deltas):
        c = list(m)
        for ax, d in zip(order, deltas):
            c[ax] = (c[ax] + d) % 4
        return c

    def flat(c):
        return c[0] * 16 + c[1] * 4 + c[2]

    def dev(c, core_id):
        return {'pp': core_id, 'ep': flat(c)}

    def far(i):
        return 1 + (2 * i) % 3

    def loop(n, step):
        lax.fori_loop(0, n, lambda i, _: (step(i), 0)[1], 0)

    fetches = [pltpu.make_async_copy(w, t, sw.at[i]) for i, (w, t) in enumerate(((wq_ref, tq_ref), (wk_ref, tk_ref), (wv_ref, tv_ref), (wo_ref, to_ref), (scale_ref, scale)))]
    for fetch in fetches:
        fetch.start()

    barrier = pltpu.get_barrier_semaphore()

    def greet(i):
        for ax in range(3):
            for cid in (core, other):
                pl.semaphore_signal(barrier, inc=1, device_id=dev(shift((ax,), (i + 1,)), cid), device_id_type=MESH)

    loop(3, greet)
    pl.semaphore_signal(barrier, inc=1, device_id=dev(m, other), device_id_type=MESH)
    pl.semaphore_wait(barrier, 19)

    def osrc(u, a, b):
        col, first, wide = UNITS[u]
        order = ORDERS[col]
        idx = [slice(None)] * 3
        idx[order[0]] = a
        idx[order[1]] = b
        return o_ref.at[idx[0], idx[1], idx[2], :, pl.ds(first, wide)]

    def remote(src, dst, send, recv, c, core_id):
        return pltpu.make_async_remote_copy(src_ref=src, dst_ref=dst, send_sem=send, recv_sem=recv, device_id=dev(c, core_id), device_id_type=MESH)

    def cp_a(u, da, db):
        order = ORDERS[UNITS[u][0]]
        c = shift(order, (da, db, 0))
        return remote(osrc(u, c[order[0]], c[order[1]]), ra[u].at[da - 1, db - 1], sa.at[u, da - 1, db], xa.at[u, da - 1, db],
                      shift(order, (da, 0, 0)), other)

    def cp_a0(u, da):
        order = ORDERS[UNITS[u][0]]
        c = shift(order, (da, 0, 0))
        return remote(osrc(u, c[order[0]], c[order[1]]), rc[u].at[:, da * 4], sa.at[u, da - 1, 0], xa.at[u, da - 1, 0], c, other)

    def cp_own(u):
        order = ORDERS[UNITS[u][0]]
        return remote(osrc(u, m[order[0]], m[order[1]]), rc[u].at[:, 0], so.at[u], xo.at[u], m, other)

    def cp_b(u, da, db):
        return remote(ra[u].at[da - 1, db - 1], rc[u].at[:, da * 4 + db], sb.at[u, da, db - 1], xb.at[u, da, db - 1],
                      shift(ORDERS[UNITS[u][0]], (0, db, 0)), core)

    def cp_b0(u, db):
        order = ORDERS[UNITS[u][0]]
        c = shift(order, (0, db, 0))
        return remote(osrc(u, c[order[0]], c[order[1]]), rc[u].at[:, db], sb.at[u, 0, db - 1], xb.at[u, 0, db - 1], c, other)

    def line(u, d):
        return shift(ORDERS[UNITS[u][0]], (0, 0, d))

    def cp_two(u, way):
        return remote(s2[u].at[pl.ds(way * half, half)], in2[u].at[way], s_two.at[u, way], x_two.at[u, way], line(u, (1, 3)[way]), core)

    def cp_one(u, way):
        return remote((s1, s3)[way][u], (in1, in3)[way][u], s_one.at[u, way], x_one.at[u, way], line(u, (1, 3)[way]), core)

    def cp_m(ax, d, k):
        src, dst = ((ids_ref, ids), (slots_ref, slots), (gates_ref, gates))[k]
        at = 0 if ax is None else 3 * ax + (4 - d)
        return remote(src, dst.at[at], sm.at[at, k], xm.at[at, k], m if ax is None else shift((ax,), (d,)), other)

    cp_h = remote(resid_ref, resid, sr, xr, m, other)

    def each_m(f):
        for k in range(3):
            f(cp_m(None, 0, k))
            for ax in range(3):
                loop(3, lambda i, ax=ax, k=k: f(cp_m(ax, i + 1, k)))

    def turn_heads(buf, n_blocks, first):
        def step(i):
            for k in range(4):
                buf[first + i * 4 + k] = jnp.swapaxes(buf[first + i * 4 + k], 0, 1)
        loop(n_blocks // 4, step)

    def choose():
        turn[...] = jnp.zeros_like(turn)

        def spread(values, dc):
            for seq in range(n_seq):
                for j in range(top_k):
                    turn[pl.ds((dc * n_seq + seq) * top_k + j, 1), 0:LENGTH] = values[seq, j].astype(f32)

        lane = lax.broadcasted_iota(jnp.int32, (LENGTH, 16 * cap), 1)
        for col in range(3):
            order = ORDERS[col]
            for dc in range(4):
                at = 3 * order[2] + dc if dc else 0
                e, slot = ids[at], slots[at]
                ec = (e >> 4, (e >> 2) & 3, e & 3)
                place = (((m[order[0]] - ec[order[0]]) & 3) * 4 + ((m[order[1]] - ec[order[1]]) & 3)) * cap + slot - flat(shift(order, (0, 0, dc))) * cap
                spread(jnp.where((slot >= 0) & (ec[order[2]] == m[order[2]]), place, -1), dc)
            pos_t = turn[...].T.astype(jnp.int32)
            for dc in range(4):
                spread(gates[3 * order[2] + dc if dc else 0], dc)
            gate_t = turn[...].T
            for dc in range(4):
                for seq in range(n_seq):
                    g = jnp.zeros((LENGTH, 16 * cap), f32)
                    for j in range(top_k):
                        at = (dc * n_seq + seq) * top_k + j
                        g = jnp.where(pos_t[0:LENGTH, at:at + 1] == lane, gate_t[0:LENGTH, at:at + 1], g)
                    for part in range(3):
                        top = jnp.minimum(g, float(jnp.finfo(bf).max)).astype(bf)
                        g_buf[col, dc, pl.ds(part * tokens + seq * LENGTH, LENGTH), :] = top
                        g = g - top.astype(f32)

    def partial(u, dc):
        col, _, wide = UNITS[u]
        rows = rc[u][line(u, dc)[ORDERS[col][2]]].reshape(16 * cap, wide)
        acc = jnp.dot(g_buf[col, dc], rows, preferred_element_type=f32)
        return (acc[:tokens] + acc[tokens:2 * tokens]) + acc[2 * tokens:]

    def send_first(us):
        loop(9, lambda i: [cp_a(u, far(i % 3), far(i // 3)).start() for u in us])
        loop(3, lambda i: [cp_a0(u, far(i)).start() for u in us])
        for u in us:
            cp_own(u).start()
        loop(3, lambda i: [cp_b0(u, far(i)).start() for u in us])

    def pass_on(us):
        def step(i):
            for u in us:
                cp_a(u, far(i % 3), far(i // 3)).wait_recv()
                cp_b(u, far(i % 3), far(i // 3)).start()
        loop(9, step)

    def rows_landed(us):
        for u in us:
            cp_own(u).wait_recv()
        loop(3, lambda i: [cp_a0(u, i + 1).wait_recv() for u in us])
        loop(3, lambda i: [cp_b0(u, i + 1).wait_recv() for u in us])
        loop(9, lambda i: [cp_b(u, far(i // 3), far(i % 3)).wait_recv() for u in us])

    def ring_start(us):
        def send(u):
            for way in range(2):
                cp_two(u, way).start()
        for k, u in enumerate(us):
            s2[u][...] = partial(u, 2)
            if k:
                send(us[k - 1])
        for k, u in enumerate(us):
            s1[u][...] = partial(u, 1)
            if k == 0:
                send(us[-1])
        for u in us:
            s3[u][...] = partial(u, 3)
        for u in us:
            cols = pl.ds(UNITS[u][1], UNITS[u][2])
            own_buf[:, cols] = resid[:, cols].astype(f32) + partial(u, 0)

    def ring_next(us):
        for u in us:
            cp_two(u, 0).wait_recv()
            cp_two(u, 1).wait_recv()
            s1[u][0:half] = s1[u][0:half] + in2[u][0]
            s3[u][half:] = s3[u][half:] + in2[u][1]
        for u in us:
            for way in range(2):
                cp_one(u, way).start()

    def own_sums(us):
        for u in us:
            _, first, wide = UNITS[u]
            cp_one(u, 0).wait_recv()
            cp_one(u, 1).wait_recv()
            y_buf[:, pl.ds(first, wide)] = ((own_buf[:, pl.ds(first, wide)] + in1[u][...]) + in3[u][...]).astype(bf)

    def first_left(us):
        loop(9, lambda i: [cp_a(u, 1 + i // 3, 1 + i % 3).wait_send() for u in us])
        loop(3, lambda i: [cp_a0(u, 1 + i).wait_send() for u in us])
        loop(3, lambda i: [cp_b0(u, 1 + i).wait_send() for u in us])
        for u in us:
            cp_own(u).wait_send()

    def second_left(us):
        loop(9, lambda i: [cp_b(u, 1 + i // 3, 1 + i % 3).wait_send() for u in us])

    def ring_left(us):
        for u in us:
            for way in range(2):
                cp_two(u, way).wait_send()
                cp_one(u, way).wait_send()

    early, late = (0, 1, 2), (3, 4, 5)
    send_first(early)
    each_m(lambda c: c.start())
    cp_h.start()
    fetches[0].wait()
    turn_heads(tq_ref, 128, 0)
    pass_on(early)
    send_first(late)
    each_m(lambda c: c.wait_recv())
    choose()
    fetches[1].wait()
    turn_heads(tk_ref, 128, 0)
    fetches[2].wait()
    turn_heads(tv_ref, 128, 0)
    cp_h.wait_recv()
    rows_landed(early)
    ring_start(early)
    pass_on(late)
    ring_next(early)
    cp_h.wait_send()
    each_m(lambda c: c.wait_send())
    first_left(early + late)
    second_left(early)
    rows_landed(late)
    ring_start(late)
    own_sums(early)
    ring_next(late)
    second_left(late)
    ring_left(early)
    own_sums(late)
    fetches[3].wait()
    fetches[4].wait()

    r = y_buf[...].astype(f32)
    x_buf[...] = (r * lax.rsqrt(jnp.mean(r * r, axis=-1, keepdims=True) + NORM_EPS) * scale[...]).astype(bf)

    t_row = lax.broadcasted_iota(jnp.int32, (tokens, tokens), 0)
    t_col = lax.broadcasted_iota(jnp.int32, (tokens, tokens), 1)
    keep = (t_row >= t_col) & (t_row // LENGTH == t_col // LENGTH)
    def project(n):
        x = x_buf[...]
        heads = [jnp.concatenate([t[:, 2 * n].reshape(width, 128), t[:, 2 * n + 1].reshape(width, 128)], axis=1) for t in (tq_ref, tk_ref, tv_ref)]
        return [jnp.dot(x, w, preferred_element_type=f32).astype(bf) for w in heads]

    def weigh(q, k):
        out = []
        for h in range(2):
            lanes = slice(h * 128, h * 128 + 128)
            s = lax.dot_general(q[:, lanes], k[:, lanes], (((1,), (1,)), ((), ())), preferred_element_type=f32) * 128 ** -0.5
            s = jnp.where(keep, s, -1e30)
            e = jnp.exp(s - jnp.max(s, axis=-1, keepdims=True))
            out.append((e.astype(bf), jnp.sum(e, axis=-1, keepdims=True)))
        return out

    def mix(n, weights, v):
        for h, (e, total) in enumerate(weights):
            mixed = jnp.dot(e, v[:, h * 128:h * 128 + 128], preferred_element_type=f32)
            a_buf[:, pl.ds((2 * n + h) * 128, 128)] = (mixed / total).astype(bf)

    q, k, v = project(0)
    held = None
    for n in range(8):
        ahead = project(n + 1) if n < 7 else None
        weights = weigh(q, k)
        if held is not None:
            mix(n - 1, *held)
        held = (weights, v)
        if ahead is not None:
            q, k, v = ahead
    mix(7, *held)

    for n in range(width // 512):
        cols = pl.ds(n * 512, 512)
        proj = jnp.dot(a_buf[...], to_ref[:, cols], preferred_element_type=f32).astype(bf)
        z_ref[:, cols] = (y_buf[:, cols].astype(f32) + proj.astype(f32)).astype(bf)

    ring_left(late)


def run_stage(o, ids, slots, gates, resid, scale, wq, wk, wv, wo):
    bf, f32 = jnp.bfloat16, jnp.float32
    cap, width = o.shape[3:]
    tokens = resid.shape[0]
    dma, buf = pltpu.SemaphoreType.DMA, pltpu.VMEM
    hbm, vmem = pl.BlockSpec(memory_space=pl.ANY), pl.BlockSpec(memory_space=pltpu.VMEM)
    sums = [buf((tokens, w), f32) for _, _, w in UNITS]
    pairs = [buf((2, tokens // 2, w), f32) for _, _, w in UNITS]
    sems = [dma((6, 3, 4)), dma((6, 3, 4)), dma((6,)), dma((6,)), dma((6, 4, 3)), dma((6, 4, 3)), dma((6, 2)), dma((6, 2)), dma((6, 2)), dma((6, 2)),
            dma((10, 3)), dma((10, 3)), dma(()), dma(()), dma((5,))]
    return pl.pallas_call(
        stage_kernel,
        out_shape=pltpu.VMEM((tokens, width), bf),
        in_specs=[hbm] * 10,
        out_specs=vmem,
        scratch_shapes=[buf(wq.shape, bf)] * 3 + [buf(wo.shape, bf), buf(scale.shape, f32)]
        + [buf((10,) + ids.shape, ids.dtype), buf((10,) + slots.shape, slots.dtype), buf((10,) + gates.shape, gates.dtype), buf(resid.shape, bf), buf(resid.shape, f32)]
        + [buf((3, 4, 3 * tokens, 16 * cap), bf)] + [buf((tokens, width), bf)] * 3 + [buf((128, 128), f32)]
        + [[buf((3, 3, 4, cap, w), bf) for _, _, w in UNITS], [buf((4, 16, cap, w), bf) for _, _, w in UNITS]]
        + [sums, sums, sums, sums, pairs, sums] + [sems],
        compiler_params=pltpu.CompilerParams(collective_id=0, has_side_effects=True, vmem_limit_bytes=63 * 2**20),
    )(o, ids, slots, gates, resid, scale, wq, wk, wv, wo)


def solution(mesh):
    token_spec = P(('data', 'pp'), 'ep', None, None)
    weight_spec = P('pp', None, None, None)

    def body(expert_out, expert_ids, slot_ids, gate_vals, residual, norm_scale, w_query, w_key, w_value, w_out):
        width = expert_out.shape[-1]
        cap = expert_out.shape[2] // 64
        seqs, length, top_k = expert_ids.shape[1:]
        ids, slots, gates = [jnp.transpose(a, (1, 3, 0, 2)) for a in (expert_ids, slot_ids, gate_vals)]
        result = run_stage(expert_out[0, 0].reshape(4, 4, 4, cap, width), ids, slots, gates, residual[0].reshape(-1, width),
                           norm_scale, *[w[0].reshape(width // 16, 16, 16, 128) for w in (w_query, w_key, w_value)], w_out[0].reshape(width, width))
        return result.reshape(residual.shape)

    return jax.shard_map(body, mesh=mesh, in_specs=(token_spec, token_spec, token_spec, token_spec, token_spec, P('pp', None), weight_spec, weight_spec, weight_spec, weight_spec), out_specs=token_spec, check_vma=False)
```
